32 devices in a mesh: dp: 1 (over z), sp: 32 (over x, y, core).
Axes of the slice: x: 4, y: 4, z: 1, core: 2. Of those that a mesh axis runs over, the one named last changes fastest.
The devices are a block of a 4x4x8 slice.
Arguments:
- q: bfloat16 [32, 16, 128], P('dp')
- k: bfloat16 [32, 8192, 16, 128], P('dp', 'sp')
- v: bfloat16 [32, 8192, 16, 128], P('dp', 'sp')
Outputs:
- q: bfloat16 [32, 16, 128], P('dp')
All inputs are finite; a program needn't handle non-finite values.
Results may differ from the reference program's by a relative error of at most 0.012.
Values are sent between devices in bfloat16 or wider.
A program may use at most 768 MiB of HBM per device.

```python
import jax
import jax.numpy as jnp

BATCH = 32
CACHE = 8192
HEADS = 16
KV_HEADS = 16
HEAD = 128


def setup_inputs(seed: int = 0, part: int = 0) -> dict:
    kq, kk, kv = (jax.random.fold_in(k, part) for k in jax.random.split(jax.random.key(seed), 3))
    return {
        "q": (3 * jax.random.normal(kq, (BATCH, HEADS, HEAD), jnp.float32)).astype(jnp.bfloat16),
        "k": jax.random.normal(kk, (BATCH, CACHE, KV_HEADS, HEAD), jnp.float32).astype(jnp.bfloat16),
        "v": jax.random.normal(kv, (BATCH, CACHE, KV_HEADS, HEAD), jnp.float32).astype(jnp.bfloat16),
    }


def einsum(form, a, b):
    return jnp.einsum(form, a.astype(jnp.float32), b.astype(jnp.float32))


def reference(q, k, v):
    grouped = q.reshape(BATCH, KV_HEADS, -1, HEAD)
    scores = einsum("bgsd,bugd->bgsu", grouped, k) * HEAD**-0.5
    weights = jax.nn.softmax(scores, -1).astype(jnp.bfloat16)
    return einsum("bgsu,bugd->bgsd", weights, v).astype(jnp.bfloat16).reshape(BATCH, HEADS, HEAD)
```

```python
import functools

import jax
import jax.numpy as jnp
from jax import lax
from jax.experimental import pallas as pl
from jax.experimental.pallas import tpu as pltpu
from jax.sharding import PartitionSpec as P

MESH = pl.DeviceIdType.MESH
LANES = 128
CORES = 2
SLOTS = 10
GROUP = 4
LAG = 4
LOW = -1e30


def scores(q, k):
    heads = q.shape[0]
    each = LANES // heads
    tiled = jnp.concatenate([q] * each, 0)
    full = lax.dot_general(k, tiled, (((1,), (1,)), ((), ())), preferred_element_type=jnp.float32)
    full = full.reshape(-1, each, heads, LANES)
    lane = lax.broadcasted_iota(jnp.int32, (1, heads, LANES), 2)
    row = lax.broadcasted_iota(jnp.int32, (1, heads, LANES), 1)
    own = full[:, 0]
    for token in range(1, each):
        own = jnp.where(lane // heads == token, full[:, token], own)
    return jnp.where(lane % heads == row, own, LOW)


def kernel(n, q_hbm, k_hbm, v_hbm, o_ref, q_ref, kbuf, vbuf, sbuf, pbuf, o32, o16, m_ref, l_ref, d16, dm, dl, x16, xst, qsem, ksem, vsem, d_send, d_recv, x_send, x_recv, r_send, r_recv):
    N, heads, head = q_ref.shape
    scale = head**-0.5
    half = heads // CORES
    rounds = N // GROUP
    me = lax.axis_index("sp")
    chips = n // CORES
    chip, core = me // CORES, lax.rem(me, CORES)
    other = 1 - core
    partner = chip * CORES + other

    def kcopy(i):
        return pltpu.make_async_copy(k_hbm.at[i], kbuf.at[lax.rem(i, SLOTS)], ksem.at[lax.rem(i, SLOTS)])

    def vcopy(i):
        return pltpu.make_async_copy(v_hbm.at[i], vbuf.at[lax.rem(i, SLOTS)], vsem.at[lax.rem(i, SLOTS)])

    qcopy = pltpu.make_async_copy(q_hbm, q_ref, qsem)
    qcopy.start()
    for i in range(SLOTS + 2):
        if i < SLOTS:
            kcopy(i).start()
        if i >= 2:
            vcopy(i - 2).start()

    barrier = pltpu.get_barrier_semaphore()

    def greet(r, _):
        pl.semaphore_signal(barrier, inc=1, device_id={"sp": lax.rem(chip + r, chips) * CORES + core}, device_id_type=MESH)
        return 0

    lax.fori_loop(1, chips, greet, 0)
    pl.semaphore_signal(barrier, inc=1, device_id={"sp": partner}, device_id_type=MESH)

    def score(i):
        sbuf[lax.rem(i, 2)] = scores(q_ref[i], kbuf[lax.rem(i, SLOTS)])

    def soften(i):
        s = sbuf[lax.rem(i, 2)]
        high = jnp.max(jnp.max(s, 0), -1, keepdims=True)
        w = jnp.exp((s - high[None]) * scale)
        total = jnp.sum(jnp.sum(w, 0), -1, keepdims=True)
        pbuf[lax.rem(i, 2)] = w.astype(jnp.bfloat16)
        m_ref[i] = jnp.broadcast_to(high * scale, (heads, LANES)).reshape(CORES, half, LANES)
        l_ref[i] = jnp.broadcast_to(total, (heads, LANES)).reshape(CORES, half, LANES)

    def weigh(i):
        w = pbuf[lax.rem(i, 2)]
        w = jnp.concatenate([w[b] for b in range(w.shape[0])], 1)
        return jnp.dot(w, vbuf[lax.rem(i, SLOTS)], preferred_element_type=jnp.float32)

    def keep(i, o):
        o = o.reshape(CORES, half, head)
        o32[i] = o
        o16[i] = o.astype(jnp.bfloat16)

    def pair(g):
        run = pl.ds(g * GROUP, GROUP)
        return [
            pltpu.make_async_remote_copy(src.at[run, other], dst.at[run], d_send.at[g, j], d_recv.at[g, j], device_id={"sp": partner}, device_id_type=MESH)
            for j, (src, dst) in enumerate(((o16, d16), (m_ref, dm), (l_ref, dl)))
        ]

    def pair_send(g):
        for copy in pair(g):
            copy.start()

    def spread(g, r):
        to = {"sp": lax.rem(chip + r, chips) * CORES + core}
        return [
            pltpu.make_async_remote_copy(buf.at[g, chip], buf.at[g, chip], x_send.at[g, j], x_recv.at[g, j], device_id=to, device_id_type=MESH)
            for j, buf in enumerate((x16, xst))
        ]

    def chip_send(g):
        for copy in pair(g):
            copy.wait_recv()
        lane = lax.broadcasted_iota(jnp.int32, (half, LANES), 1)
        row = lax.broadcasted_iota(jnp.int32, (half, LANES), 0)
        highs = jnp.zeros((half, LANES), jnp.float32)
        totals = jnp.zeros((half, LANES), jnp.float32)
        for s in range(GROUP):
            i = g * GROUP + s
            m1, m2 = m_ref[i, core], dm[i]
            m = jnp.maximum(m1, m2)
            a1, a2 = jnp.exp(m1 - m), jnp.exp(m2 - m)
            o = o32[i, core] * a1 + d16[i].astype(jnp.float32) * a2
            l = l_ref[i, core] * a1 + dl[i] * a2
            x16[g, chip, s] = o.astype(jnp.bfloat16)
            here = lane == s * half + row
            highs = jnp.where(here, m, highs)
            totals = jnp.where(here, l, totals)
        xst[g, chip] = jnp.concatenate([jnp.sum(highs, 0, keepdims=True), jnp.sum(totals, 0, keepdims=True)], 0)

        def send(r, _):
            for copy in spread(g, r):
                copy.start()
            return 0

        lax.fori_loop(1, chips, send, 0)

    def spread_wait(g, what):
        for j, buf in enumerate((x16, xst)):
            run = buf.at[g, pl.ds(0, chips - 1)]
            pltpu.make_async_copy(run, run, what.at[g, j]).wait()

    def back(g):
        run = pl.ds(g * GROUP, GROUP)
        return pltpu.make_async_remote_copy(o_ref.at[run, core], o_ref.at[run, core], r_send.at[g], r_recv.at[g], device_id={"sp": partner}, device_id_type=MESH)

    def finish(g):
        spread_wait(g, x_recv)
        st = [xst[g, j] for j in range(chips)]
        m = functools.reduce(jnp.maximum, [s[:1] for s in st])
        w = [jnp.exp(s[:1] - m) for s in st]
        total = functools.reduce(jnp.add, [s[1:] * x for s, x in zip(st, w)])
        w = [x / total for x in w]
        lane = lax.broadcasted_iota(jnp.int32, (half, LANES), 1)
        row = lax.broadcasted_iota(jnp.int32, (half, LANES), 0)
        for s in range(GROUP):
            o = jnp.zeros((half, head), jnp.float32)
            for j in range(chips):
                f = jnp.sum(jnp.where(lane == s * half + row, w[j], 0.0), -1, keepdims=True)
                o = o + x16[g, j, s].astype(jnp.float32) * f
            o_ref[g * GROUP + s, core] = o.astype(jnp.bfloat16)
        back(g).start()

    kcopy(0).wait()
    qcopy.wait()
    score(0)
    kcopy(1).wait()
    score(1)
    soften(0)
    pl.semaphore_wait(barrier, chips)

    def refill_k(i):
        @pl.when(i + SLOTS < N)
        def _():
            kcopy(i + SLOTS).start()

    def refill_v(i):
        @pl.when(i + SLOTS < N)
        def _():
            vcopy(i + SLOTS).start()

    refill_k(0)
    refill_k(1)

    def step(i, _):
        kcopy(i + 2).wait()
        vcopy(i).wait()
        s = scores(q_ref[i + 2], kbuf[lax.rem(i + 2, SLOTS)])
        o = weigh(i)
        soften(i + 1)
        sbuf[lax.rem(i, 2)] = s
        keep(i, o)
        refill_k(i + 2)
        refill_v(i)

        @pl.when(lax.rem(i, GROUP) == GROUP - 1)
        def _():
            g = i // GROUP
            pair_send(g)

            @pl.when(g >= 1)
            def _():
                chip_send(g - 1)

            @pl.when(g >= LAG)
            def _():
                finish(g - LAG)

        return 0

    lax.fori_loop(0, N - 2, step, 0)
    vcopy(N - 2).wait()
    o = weigh(N - 2)
    soften(N - 1)
    keep(N - 2, o)
    vcopy(N - 1).wait()
    keep(N - 1, weigh(N - 1))
    last = rounds - 1
    pair_send(last)
    chip_send(last - 1)
    chip_send(last)

    def rest(g, _):
        finish(g)
        return 0

    lax.fori_loop(max((N - 2) // GROUP - LAG, 0), rounds, rest, 0)

    def drain(g, _):
        back(g).wait()
        for copy in pair(g):
            copy.wait_send()
        spread_wait(g, x_send)
        return 0

    lax.fori_loop(0, rounds, drain, 0)


def solution(mesh):
    n = mesh.shape["sp"]

    def step(q, k, v):
        N, tokens, heads, head = k.shape
        half = heads // CORES
        rounds = N // GROUP
        chips = n // CORES
        blocks = tokens * heads // LANES
        flat = (N, tokens * heads, head)
        bf16, f32 = jnp.bfloat16, jnp.float32
        out = pl.pallas_call(
            functools.partial(kernel, n),
            out_shape=jax.ShapeDtypeStruct((N, CORES, half, head), bf16),
            in_specs=[pl.BlockSpec(memory_space=pl.ANY)] * 3,
            out_specs=pl.BlockSpec(memory_space=pltpu.VMEM),
            scratch_shapes=[
                pltpu.VMEM((N, heads, head), bf16),
                pltpu.VMEM((SLOTS, tokens * heads, head), bf16),
                pltpu.VMEM((SLOTS, tokens * heads, head), bf16),
                pltpu.VMEM((2, blocks, heads, LANES), f32),
                pltpu.VMEM((2, blocks, heads, LANES), bf16),
                pltpu.VMEM((N, CORES, half, head), f32),
                pltpu.VMEM((N, CORES, half, head), bf16),
                pltpu.VMEM((N, CORES, half, LANES), f32),
                pltpu.VMEM((N, CORES, half, LANES), f32),
                pltpu.VMEM((N, half, head), bf16),
                pltpu.VMEM((N, half, LANES), f32),
                pltpu.VMEM((N, half, LANES), f32),
                pltpu.VMEM((rounds, chips, GROUP, half, head), bf16),
                pltpu.VMEM((rounds, chips, 2, LANES), f32),
                pltpu.SemaphoreType.DMA(()),
                pltpu.SemaphoreType.DMA((SLOTS,)),
                pltpu.SemaphoreType.DMA((SLOTS,)),
                pltpu.SemaphoreType.DMA((rounds, 3)),
                pltpu.SemaphoreType.DMA((rounds, 3)),
                pltpu.SemaphoreType.DMA((rounds, 2)),
                pltpu.SemaphoreType.DMA((rounds, 2)),
                pltpu.SemaphoreType.DMA((rounds,)),
                pltpu.SemaphoreType.DMA((rounds,)),
            ],
            compiler_params=pltpu.CompilerParams(collective_id=0, has_side_effects=True, vmem_limit_bytes=60 * 2**20),
        )(q, k.reshape(flat), v.reshape(flat))
        return out.reshape(q.shape)

    return jax.shard_map(
        step,
        mesh=mesh,
        in_specs=(P("dp", None, None), P("dp", "sp", None, None), P("dp", "sp", None, None)),
        out_specs=P("dp", None, None),
        check_vma=False,
    )
```

```python
import functools

import jax
import jax.numpy as jnp
from jax import lax
from jax.experimental import pallas as pl
from jax.experimental.pallas import tpu as pltpu
from jax.sharding import PartitionSpec as P

MESH = pl.DeviceIdType.MESH
LANES, ROWS = 128, 8
SLOTS = 8
STEP = 2
LAST = 4
HOLD = 12
LOW = -1e30
ABL = 0
AHEAD = 6


def kernel(n, q_hbm, k_hbm, v_hbm, o_ref, q_ref, kbuf, vbuf, sbuf, pbuf, st_ref, msg, inbox, x16, xst, qsem, ksem, vsem, p_send, p_recv, b_send, b_recv, x_send, x_recv):
    N, heads, head = q_ref.shape
    scale = head**-0.5
    halves = heads // ROWS
    owned = N - LAST
    me = lax.axis_index("sp")

    def kcopy(i):
        return pltpu.make_async_copy(k_hbm.at[i], kbuf.at[lax.rem(i, SLOTS)], ksem.at[lax.rem(i, SLOTS)])

    def vcopy(i):
        return pltpu.make_async_copy(v_hbm.at[i], vbuf.at[lax.rem(i, SLOTS)], vsem.at[lax.rem(i, SLOTS)])

    qcopy = pltpu.make_async_copy(q_hbm, q_ref, qsem)
    qcopy.start(priority=1)
    first = [kcopy(i) for i in range(2 * STEP)]
    for i in range(SLOTS):
        first.append(vcopy(i))
        if i + 2 * STEP < SLOTS:
            first.append(kcopy(i + 2 * STEP))
    for copy in first[:AHEAD]:
        copy.start(priority=1)

    barrier = pltpu.get_barrier_semaphore()

    def peer(r):
        return {"sp": lax.rem(me + r, n)}

    def greet(r, _):
        pl.semaphore_signal(barrier, inc=1, device_id=peer(r), device_id_type=MESH)
        return 0

    lax.fori_loop(1, n, greet, 0)

    lane = lax.broadcasted_iota(jnp.int32, (ROWS, LANES), 1)
    each = LANES // 2 // halves

    def score(i):
        return lax.dot_general(q_ref[i], kbuf[lax.rem(i, SLOTS)], (((1,), (1,)), ((), ())), preferred_element_type=jnp.float32)

    def soften(i):
        s = sbuf[lax.rem(i, 2 * STEP)]
        places = lax.broadcasted_iota(jnp.int32, s.shape, 1)
        rows = lax.broadcasted_iota(jnp.int32, s.shape, 0)
        s = jnp.where(places % heads == rows, s, LOW)
        high = jnp.max(s, -1, keepdims=True)
        w = jnp.exp((s - high) * scale)
        total = jnp.sum(w, -1, keepdims=True)
        pbuf[lax.rem(i, 2 * STEP)] = w.astype(jnp.bfloat16)
        tile = jnp.zeros((ROWS, LANES), jnp.float32)
        for h in range(halves):
            run = slice(h * ROWS, (h + 1) * ROWS)
            tile = jnp.where(lane == h * each, high[run] * scale, tile)
            tile = jnp.where(lane == LANES // 2 + h * each, total[run], tile)
        st_ref[i] = tile

    def weigh(i):
        return jnp.dot(pbuf[lax.rem(i, 2 * STEP)], vbuf[lax.rem(i, SLOTS)], preferred_element_type=jnp.float32)

    def keep(i, o):
        msg[i, :halves] = o.reshape(halves, ROWS, head)
        msg[i, halves] = st_ref[i]

    def keep_last(i, o):
        x16[me, i - owned] = o.reshape(halves, ROWS, head).astype(jnp.bfloat16)
        here = st_ref[i] if i == owned else pltpu.roll(st_ref[i], i - owned, 1)
        xst[me] = here if i == owned else jnp.where(lane % each == i - owned, here, xst[me])

    def merge(count, part, tiles):
        high = functools.reduce(jnp.maximum, tiles)
        ws = [jnp.exp(t - high) for t in tiles]
        total = functools.reduce(jnp.add, [pltpu.roll(t, LANES // 2, 1) * w for t, w in zip(tiles, ws)])
        fs = [w / total for w in ws]
        return [
            jnp.stack([functools.reduce(jnp.add, [part(j, s, h).astype(jnp.float32) * f[:, h * each + s : h * each + s + 1] for j, f in enumerate(fs)]) for h in range(halves)])
            for s in range(count)
        ]

    def to_owner(i):
        return pltpu.make_async_remote_copy(msg.at[i], inbox.at[me], p_send.at[i], p_recv, device_id={"sp": i}, device_id_type=MESH)

    def send_part(i):
        @pl.when(i != me)
        def _():
            to_owner(i).start()

    def spread(ref, sem, j):
        return lambda r: pltpu.make_async_remote_copy(ref, ref, x_send.at[j], sem, device_id=peer(r), device_id_type=MESH)

    def all_of(ref, sem):
        run = ref.at[pl.ds(0, n - 1)]
        pltpu.make_async_copy(run, run, sem).wait()

    def result_copy(r):
        return pltpu.make_async_remote_copy(o_ref.at[me], o_ref.at[me], b_send, b_recv.at[me], device_id=peer(r), device_id_type=MESH)

    def own():
        inbox[me] = msg[me]
        all_of(inbox, p_recv)
        o_ref[me] = merge(1, lambda j, s, h: inbox[j, h], [inbox[j, halves] for j in range(n)])[0].astype(jnp.bfloat16)

        def send(r, _):
            result_copy(r).start()
            return 0

        lax.fori_loop(1, n, send, 0)

    for i in range(2 * STEP):
        kcopy(i).wait()
        if i == 0:
            qcopy.wait()
        rest = len(first) - AHEAD
        for copy in first[AHEAD + rest * i // (2 * STEP) : AHEAD + rest * (i + 1) // (2 * STEP)]:
            copy.start(priority=1)
        sbuf[i] = score(i)
        if i < STEP:
            soften(i)

    def refill(copy, i):
        @pl.when(i + SLOTS < N)
        def _():
            copy(i + SLOTS).start(priority=1)

    for i in range(2 * STEP):
        refill(kcopy, i)

    def step(t, _):
        i = t * STEP
        for u in range(STEP):
            kcopy(i + 2 * STEP + u).wait()
            vcopy(i + u).wait()
        os = [weigh(i + u) for u in range(STEP)]
        ss = [score(i + 2 * STEP + u) for u in range(STEP)]
        for u in range(STEP):
            soften(i + STEP + u)
        for u in range(STEP):
            sbuf[lax.rem(i + u, 2 * STEP)] = ss[u]
            keep(i + u, os[u])
        for u in range(STEP):
            refill(kcopy, i + 2 * STEP + u)
            refill(vcopy, i + u)
        if ABL:
            return 0

        @pl.when(i == HOLD)
        def _():
            pl.semaphore_wait(barrier, n - 1)

            def send(j, _):
                send_part(j)
                return 0

            lax.fori_loop(0, HOLD, send, 0)

        @pl.when(i >= HOLD)
        def _():
            for u in range(STEP):
                send_part(i + u)

        return 0

    lax.fori_loop(0, (N - 2 * STEP) // STEP, step, 0)
    for i in range(N - 2 * STEP, N):
        if i < N - STEP:
            soften(i + STEP)
        vcopy(i).wait()
        o = weigh(i)
        if i < owned:
            keep(i, o)
            if not ABL:
                send_part(i)
        else:
            keep_last(i, o)
    if ABL:
        pl.semaphore_wait(barrier, n - 1)
        return

    def send_last(r, _):
        for j, (ref, sem) in enumerate(((x16.at[me], x_recv.at[0]), (xst.at[me], x_recv.at[1]))):
            spread(ref, sem, j)(r).start()
        return 0

    lax.fori_loop(1, n, send_last, 0)
    pl.when(me < owned)(own)
    all_of(x16, x_recv.at[0])
    all_of(xst, x_recv.at[1])
    for s, o in enumerate(merge(LAST, lambda j, s, h: x16[j, s, h], [xst[j] for j in range(n)])):
        o_ref[owned + s] = o.astype(jnp.bfloat16)

    def drain(i, _):
        @pl.when(i != me)
        def _():
            to_owner(i).wait_send()
            pltpu.make_async_copy(o_ref.at[i], o_ref.at[i], b_recv.at[i]).wait()

        return 0

    lax.fori_loop(0, owned, drain, 0)

    @pl.when(me < owned)
    def _():
        all_of(o_ref, b_send)

    all_of(x16, x_send.at[0])
    all_of(xst, x_send.at[1])


def solution(mesh):
    n = mesh.shape["sp"]

    def step(q, k, v):
        N, tokens, heads, head = k.shape
        halves = heads // ROWS
        flat = (N, tokens * heads, head)
        bf16, f32 = jnp.bfloat16, jnp.float32
        dma = pltpu.SemaphoreType.DMA
        out = pl.pallas_call(
            functools.partial(kernel, n),
            out_shape=pltpu.VMEM((N, halves, ROWS, head), bf16),
            in_specs=[pl.BlockSpec(memory_space=pl.ANY)] * 3,
            out_specs=pl.BlockSpec(memory_space=pltpu.VMEM),
            scratch_shapes=[
                pltpu.VMEM((N, heads, head), bf16),
                pltpu.VMEM((SLOTS, tokens * heads, head), bf16),
                pltpu.VMEM((SLOTS, tokens * heads, head), bf16),
                pltpu.VMEM((2 * STEP, heads, tokens * heads), f32),
                pltpu.VMEM((2 * STEP, heads, tokens * heads), bf16),
                pltpu.VMEM((N, ROWS, LANES), f32),
                pltpu.VMEM((N, halves + 1, ROWS, LANES), f32),
                pltpu.VMEM((n, halves + 1, ROWS, LANES), f32),
                pltpu.VMEM((n, LAST, halves, ROWS, head), bf16),
                pltpu.VMEM((n, ROWS, LANES), f32),
                dma(()),
                dma((SLOTS,)),
                dma((SLOTS,)),
                dma((N,)),
                dma(()),
                dma(()),
                dma((N,)),
                dma((2,)),
                dma((2,)),
            ],
            compiler_params=pltpu.CompilerParams(collective_id=0, has_side_effects=True, vmem_limit_bytes=60 * 2**20),
        )(q, k.reshape(flat), v.reshape(flat))
        return out.reshape(q.shape)

    return jax.shard_map(
        step,
        mesh=mesh,
        in_specs=(P("dp", None, None), P("dp", "sp", None, None), P("dp", "sp", None, None)),
        out_specs=P("dp", None, None),
        check_vma=False,
    )
```

```python
import functools

import jax
import jax.numpy as jnp
from jax import lax
from jax.experimental import pallas as pl
from jax.experimental.pallas import tpu as pltpu
from jax.sharding import PartitionSpec as P

MESH = pl.DeviceIdType.MESH
LANES, ROWS = 128, 8
KEYS, SLOTS = 8, 8
STEP = 2
LAST = 3
HOLD = 12
LOW = -1e30
LEAD = 4
AHEAD = 6


def kernel(n, q_hbm, k_hbm, v_hbm, o_ref, q_ref, kbuf, vbuf, sbuf, pbuf, st_ref, msg, inbox, x16, xst, qsem, ksem, vsem, p_send, p_recv, b_send, b_recv, x_send, x_recv):
    N, heads, head = q_ref.shape
    scale = head**-0.5
    halves = heads // ROWS
    owned = N - LAST
    me = lax.axis_index("sp")

    def kcopy(i):
        return pltpu.make_async_copy(k_hbm.at[i], kbuf.at[lax.rem(i, KEYS)], ksem.at[lax.rem(i, KEYS)])

    def vcopy(i):
        return pltpu.make_async_copy(v_hbm.at[i], vbuf.at[lax.rem(i, SLOTS)], vsem.at[lax.rem(i, SLOTS)])

    qcopy = pltpu.make_async_copy(q_hbm, q_ref, qsem)
    qcopy.start(priority=1)
    first = [kcopy(i) for i in range(LEAD)]
    for i in range(max(SLOTS, KEYS - LEAD)):
        if i < SLOTS:
            first.append(vcopy(i))
        if i + LEAD < KEYS:
            first.append(kcopy(i + LEAD))
    for copy in first[:AHEAD]:
        copy.start(priority=1)

    barrier = pltpu.get_barrier_semaphore()

    def peer(r):
        return {"sp": r - 1 + jnp.where(r > me, 1, 0)}

    def greet(r, _):
        pl.semaphore_signal(barrier, inc=1, device_id=peer(r), device_id_type=MESH)
        return 0

    lax.fori_loop(1, n, greet, 0)

    lane = lax.broadcasted_iota(jnp.int32, (ROWS, LANES), 1)
    each = LANES // 2 // halves

    def score(i):
        return lax.dot_general(q_ref[i], kbuf[lax.rem(i, KEYS)], (((1,), (1,)), ((), ())), preferred_element_type=jnp.float32)

    def soften(i):
        s = sbuf[lax.rem(i, 2 * STEP)]
        places = lax.broadcasted_iota(jnp.int32, s.shape, 1)
        rows = lax.broadcasted_iota(jnp.int32, s.shape, 0)
        s = jnp.where(places % heads == rows, s, LOW)
        high = jnp.max(s, -1, keepdims=True)
        w = jnp.exp((s - high) * scale)
        total = jnp.sum(w, -1, keepdims=True)
        pbuf[lax.rem(i, LEAD)] = w.astype(jnp.bfloat16)
        tile = jnp.zeros((ROWS, LANES), jnp.float32)
        for h in range(halves):
            run = slice(h * ROWS, (h + 1) * ROWS)
            tile = jnp.where(lane == h * each, high[run] * scale, tile)
            tile = jnp.where(lane == LANES // 2 + h * each, total[run], tile)
        st_ref[i] = tile

    def weigh(i):
        return jnp.dot(pbuf[lax.rem(i, LEAD)], vbuf[lax.rem(i, SLOTS)], preferred_element_type=jnp.float32)

    def keep(i, o):
        msg[i, :halves] = o.reshape(halves, ROWS, head)
        msg[i, halves] = st_ref[i]

    def keep_last(i, o):
        x16[me, i - owned] = o.reshape(halves, ROWS, head).astype(jnp.bfloat16)
        here = st_ref[i] if i == owned else pltpu.roll(st_ref[i], i - owned, 1)
        xst[me] = here if i == owned else jnp.where(lane % each == i - owned, here, xst[me])

    def merge(count, part, tiles):
        high = functools.reduce(jnp.maximum, tiles)
        ws = [jnp.exp(t - high) for t in tiles]
        total = functools.reduce(jnp.add, [pltpu.roll(t, LANES // 2, 1) * w for t, w in zip(tiles, ws)])
        fs = [w / total for w in ws]
        return [
            jnp.stack([functools.reduce(jnp.add, [part(j, s, h).astype(jnp.float32) * f[:, h * each + s : h * each + s + 1] for j, f in enumerate(fs)]) for h in range(halves)])
            for s in range(count)
        ]

    def to_owner(i):
        return pltpu.make_async_remote_copy(msg.at[i], inbox.at[me], p_send, p_recv, device_id={"sp": i}, device_id_type=MESH)

    def send_part(i):
        @pl.when(i != me)
        def _():
            to_owner(i).start()

    def spread(ref, sem, j):
        return lambda r: pltpu.make_async_remote_copy(ref, ref, x_send.at[j], sem, device_id=peer(r), device_id_type=MESH)

    def all_of(ref, sem):
        run = ref.at[pl.ds(0, n - 1)]
        pltpu.make_async_copy(run, run, sem).wait()

    def result_copy(r):
        return pltpu.make_async_remote_copy(o_ref.at[me], o_ref.at[me], b_send, b_recv, device_id=peer(r), device_id_type=MESH)

    def own():
        inbox[me] = msg[me]
        all_of(inbox, p_recv)
        o_ref[me] = merge(1, lambda j, s, h: inbox[j, h], [inbox[j, halves] for j in range(n)])[0].astype(jnp.bfloat16)

        def send(r, _):
            result_copy(r).start()
            return 0

        lax.fori_loop(1, n, send, 0)

    def refill(copy, i, slots):
        @pl.when(i + slots < N)
        def _():
            copy(i + slots).start(priority=1)

    def score_step(i):
        for u in range(STEP):
            kcopy(i + u).wait()
        return [score(i + u) for u in range(STEP)]

    def hold(i, ss):
        for u in range(STEP):
            sbuf[lax.rem(i + u, 2 * STEP)] = ss[u]

    kcopy(0).wait()
    qcopy.wait()
    for copy in first[AHEAD:]:
        copy.start(priority=1)
    kcopy(1).wait()
    hold(0, [score(u) for u in range(STEP)])

    def early(t, _):
        i = t * STEP
        ss = score_step(i)
        for u in range(STEP):
            soften(i - STEP + u)
        hold(i, ss)
        for u in range(STEP):
            refill(kcopy, i - STEP + u, KEYS)
        return 0

    lax.fori_loop(1, LEAD // STEP, early, 0)
    for u in range(STEP):
        refill(kcopy, LEAD - STEP + u, KEYS)

    def step(t, _):
        i = t * STEP
        for u in range(STEP):
            kcopy(i + LEAD + u).wait()
            vcopy(i + u).wait()
        os = [weigh(i + u) for u in range(STEP)]
        ss = [score(i + LEAD + u) for u in range(STEP)]
        for u in range(STEP):
            soften(i + LEAD - STEP + u)
        hold(i + LEAD, ss)
        for u in range(STEP):
            keep(i + u, os[u])
        for u in range(STEP):
            refill(kcopy, i + LEAD + u, KEYS)
            refill(vcopy, i + u, SLOTS)

        @pl.when(i == HOLD)
        def _():
            pl.semaphore_wait(barrier, n - 1)

            def send(j, _):
                send_part(j)
                return 0

            lax.fori_loop(0, HOLD, send, 0)

        @pl.when(i >= HOLD)
        def _():
            for u in range(STEP):
                send_part(i + u)

        return 0

    lax.fori_loop(0, (N - LEAD) // STEP, step, 0)
    for i in range(N - LEAD, N, STEP):
        pairs = [range(i, i + STEP)] if i + STEP < N else [range(u, u + 1) for u in range(i, N)]
        for pair in pairs:
            for u in pair:
                vcopy(u).wait()
            os = [weigh(u) for u in pair]
            if i == N - LEAD:
                for u in range(STEP):
                    soften(N - STEP + u)
            for u, o in zip(pair, os):
                if u < owned:
                    keep(u, o)
                else:
                    keep_last(u, o)
            for u in pair:
                if u < owned:
                    send_part(u)

    def send_last(r, _):
        for j, (ref, sem) in enumerate(((x16.at[me], x_recv.at[0]), (xst.at[me], x_recv.at[1]))):
            spread(ref, sem, j)(r).start()
        return 0

    lax.fori_loop(1, n, send_last, 0)
    pl.when(me < owned)(own)
    all_of(x16, x_recv.at[0])
    all_of(xst, x_recv.at[1])
    for s, o in enumerate(merge(LAST, lambda j, s, h: x16[j, s, h], [xst[j] for j in range(n)])):
        o_ref[owned + s] = o.astype(jnp.bfloat16)

    def blocks(ref, count, sem):
        run = ref.at[pl.ds(0, count)]
        pltpu.make_async_copy(run, run, sem).wait()

    @pl.when(me < owned)
    def _():
        blocks(o_ref, n - 1, b_send)
        blocks(o_ref, owned - 1, b_recv)
        blocks(msg, owned - 1, p_send)

    @pl.when(me >= owned)
    def _():
        blocks(o_ref, owned, b_recv)
        blocks(msg, owned, p_send)

    all_of(x16, x_send.at[0])
    all_of(xst, x_send.at[1])


def solution(mesh):
    n = mesh.shape["sp"]

    def step(q, k, v):
        N, tokens, heads, head = k.shape
        halves = heads // ROWS
        flat = (N, tokens * heads, head)
        bf16, f32 = jnp.bfloat16, jnp.float32
        dma = pltpu.SemaphoreType.DMA
        out = pl.pallas_call(
            functools.partial(kernel, n),
            out_shape=pltpu.VMEM((N, halves, ROWS, head), bf16),
            in_specs=[pl.BlockSpec(memory_space=pl.ANY)] * 3,
            out_specs=pl.BlockSpec(memory_space=pltpu.VMEM),
            scratch_shapes=[
                pltpu.VMEM((N, heads, head), bf16),
                pltpu.VMEM((KEYS, tokens * heads, head), bf16),
                pltpu.VMEM((SLOTS, tokens * heads, head), bf16),
                pltpu.VMEM((2 * STEP, heads, tokens * heads), f32),
                pltpu.VMEM((LEAD, heads, tokens * heads), bf16),
                pltpu.VMEM((N, ROWS, LANES), f32),
                pltpu.VMEM((N, halves + 1, ROWS, LANES), f32),
                pltpu.VMEM((n, halves + 1, ROWS, LANES), f32),
                pltpu.VMEM((n, LAST, halves, ROWS, head), bf16),
                pltpu.VMEM((n, ROWS, LANES), f32),
                dma(()),
                dma((KEYS,)),
                dma((SLOTS,)),
                *[dma(())] * 4,
                dma((2,)),
                dma((2,)),
            ],
            compiler_params=pltpu.CompilerParams(collective_id=0, has_side_effects=True, vmem_limit_bytes=60 * 2**20),
        )(q, k.reshape(flat), v.reshape(flat))
        return out.reshape(q.shape)

    return jax.shard_map(
        step,
        mesh=mesh,
        in_specs=(P("dp", None, None), P("dp", "sp", None, None), P("dp", "sp", None, None)),
        out_specs=P("dp", None, None),
        check_vma=False,
    )
```

```python
import functools

import jax
import jax.numpy as jnp
from jax import lax
from jax.experimental import pallas as pl
from jax.experimental.pallas import tpu as pltpu
from jax.sharding import PartitionSpec as P

MESH = pl.DeviceIdType.MESH
LANES, ROWS = 128, 8
KEYS, SLOTS = 8, 8
STEP = 2
LAST = 3
HOLD = 12
LOW = -1e30
LEAD = 4
AHEAD = 6


def kernel(n, q_hbm, k_hbm, v_hbm, o_ref, q_ref, kbuf, vbuf, sbuf, pbuf, st_ref, msg, inbox, x16, xst, factor, qsem, ksem, vsem, p_send, p_recv, b_send, b_recv, x_send, x_recv):
    N, heads, head = q_ref.shape
    scale = head**-0.5
    halves = heads // ROWS
    owned = N - LAST
    me = lax.axis_index("sp")

    def kcopy(i):
        return pltpu.make_async_copy(k_hbm.at[i], kbuf.at[lax.rem(i, KEYS)], ksem.at[lax.rem(i, KEYS)])

    def vcopy(i):
        return pltpu.make_async_copy(v_hbm.at[i], vbuf.at[lax.rem(i, SLOTS)], vsem.at[lax.rem(i, SLOTS)])

    qcopy = pltpu.make_async_copy(q_hbm, q_ref, qsem)
    qcopy.start(priority=1)
    first = [kcopy(i) for i in range(LEAD)]
    for i in range(max(SLOTS, KEYS - LEAD)):
        if i < SLOTS:
            first.append(vcopy(i))
        if i + LEAD < KEYS:
            first.append(kcopy(i + LEAD))
    for copy in first[:AHEAD]:
        copy.start(priority=1)

    barrier = pltpu.get_barrier_semaphore()

    def peer(r):
        return {"sp": r - 1 + jnp.where(r > me, 1, 0)}

    def greet(r, _):
        pl.semaphore_signal(barrier, inc=1, device_id=peer(r), device_id_type=MESH)
        return 0

    lax.fori_loop(1, n, greet, 0)

    lane = lax.broadcasted_iota(jnp.int32, (ROWS, LANES), 1)
    each = LANES // 2 // halves

    def score(i):
        return lax.dot_general(q_ref[i], kbuf[lax.rem(i, KEYS)], (((1,), (1,)), ((), ())), preferred_element_type=jnp.float32)

    def soften(i):
        s = sbuf[lax.rem(i, 2 * STEP)]
        places = lax.broadcasted_iota(jnp.int32, s.shape, 1)
        rows = lax.broadcasted_iota(jnp.int32, s.shape, 0)
        s = jnp.where(places % heads == rows, s, LOW)
        high = jnp.max(s, -1, keepdims=True)
        w = jnp.exp((s - high) * scale)
        total = jnp.sum(w, -1, keepdims=True)
        pbuf[lax.rem(i, LEAD)] = w.astype(jnp.bfloat16)
        tile = jnp.zeros((ROWS, LANES), jnp.float32)
        for h in range(halves):
            run = slice(h * ROWS, (h + 1) * ROWS)
            tile = jnp.where(lane == h * each, high[run] * scale, tile)
            tile = jnp.where(lane == LANES // 2 + h * each, total[run], tile)
        st_ref[i] = tile

    def weigh(i):
        return jnp.dot(pbuf[lax.rem(i, LEAD)], vbuf[lax.rem(i, SLOTS)], preferred_element_type=jnp.float32)

    def keep(i, o):
        msg[i, :halves] = o.reshape(halves, ROWS, head)
        msg[i, halves] = st_ref[i]

    def keep_last(i, o):
        x16[me, i - owned] = o.reshape(halves, ROWS, head).astype(jnp.bfloat16)

    def pack_last():
        tile = st_ref[owned]
        for s in range(1, LAST):
            tile = jnp.where(lane % each == s, pltpu.roll(st_ref[owned + s], s, 1), tile)
        xst[me] = tile

    def shares(tiles):
        high = functools.reduce(jnp.maximum, tiles)
        ws = [jnp.exp(t - high) for t in tiles]
        total = functools.reduce(jnp.add, [pltpu.roll(t, LANES // 2, 1) * w for t, w in zip(tiles, ws)])
        return [w / total for w in ws]

    def merge_own():
        fs = shares([inbox[j, halves] for j in range(n)])
        for h in range(halves):
            o = functools.reduce(jnp.add, [inbox[j, h] * f[:, h * each : h * each + 1] for j, f in enumerate(fs)])
            o_ref[me, h] = o.astype(jnp.bfloat16)

    def shares_last():
        for j, f in enumerate(shares([xst[j] for j in range(n)])):
            for s in range(LAST):
                for h in range(halves):
                    at = h * each + s
                    factor[j, s, h] = jnp.broadcast_to(f[:, at : at + 1], (ROWS, LANES))

    def merge_last():
        for s in range(LAST):
            for h in range(halves):
                o = functools.reduce(jnp.add, [x16[j, s, h].astype(jnp.float32) * factor[j, s, h] for j in range(n)])
                o_ref[owned + s, h] = o.astype(jnp.bfloat16)

    def to_owner(i):
        return pltpu.make_async_remote_copy(msg.at[i], inbox.at[me], p_send, p_recv, device_id={"sp": i}, device_id_type=MESH)

    def send_part(i):
        @pl.when(i != me)
        def _():
            to_owner(i).start()

    def spread(ref, j):
        def send(r, _):
            pltpu.make_async_remote_copy(ref.at[me], ref.at[me], x_send.at[j], x_recv.at[j], device_id=peer(r), device_id_type=MESH).start()
            return 0

        lax.fori_loop(1, n, send, 0)

    def all_of(ref, sem):
        run = ref.at[pl.ds(0, n - 1)]
        pltpu.make_async_copy(run, run, sem).wait()

    def result_copy(r):
        return pltpu.make_async_remote_copy(o_ref.at[me], o_ref.at[me], b_send, b_recv, device_id=peer(r), device_id_type=MESH)

    def own():
        inbox[me] = msg[me]
        all_of(inbox, p_recv)
        merge_own()

        def send(r, _):
            result_copy(r).start()
            return 0

        lax.fori_loop(1, n, send, 0)

    def refill(copy, i, slots):
        @pl.when(i + slots < N)
        def _():
            copy(i + slots).start(priority=1)

    def score_step(i):
        for u in range(STEP):
            kcopy(i + u).wait()
        return [score(i + u) for u in range(STEP)]

    def hold(i, ss):
        for u in range(STEP):
            sbuf[lax.rem(i + u, 2 * STEP)] = ss[u]

    kcopy(0).wait()
    qcopy.wait()
    for copy in first[AHEAD:]:
        copy.start(priority=1)
    kcopy(1).wait()
    hold(0, [score(u) for u in range(STEP)])

    def early(t, _):
        i = t * STEP
        ss = score_step(i)
        for u in range(STEP):
            soften(i - STEP + u)
        hold(i, ss)
        for u in range(STEP):
            refill(kcopy, i - STEP + u, KEYS)
        return 0

    lax.fori_loop(1, LEAD // STEP, early, 0)
    for u in range(STEP):
        refill(kcopy, LEAD - STEP + u, KEYS)

    def step(t, _):
        i = t * STEP
        for u in range(STEP):
            kcopy(i + LEAD + u).wait()
            vcopy(i + u).wait()
        os = [weigh(i + u) for u in range(STEP)]
        ss = [score(i + LEAD + u) for u in range(STEP)]
        for u in range(STEP):
            soften(i + LEAD - STEP + u)
        hold(i + LEAD, ss)
        for u in range(STEP):
            keep(i + u, os[u])
        for u in range(STEP):
            refill(kcopy, i + LEAD + u, KEYS)
            refill(vcopy, i + u, SLOTS)

        @pl.when(i == HOLD)
        def _():
            pl.semaphore_wait(barrier, n - 1)

            def send(j, _):
                send_part(j)
                return 0

            lax.fori_loop(0, HOLD, send, 0)

        @pl.when(i >= HOLD)
        def _():
            for u in range(STEP):
                send_part(i + u)

        return 0

    lax.fori_loop(0, (N - LEAD) // STEP, step, 0)
    for i in range(N - LEAD, N, STEP):
        pairs = [range(i, i + STEP)] if i + STEP <= owned else [range(u, u + 1) for u in range(i, i + STEP)]
        for pair in pairs:
            for u in pair:
                vcopy(u).wait()
            os = [weigh(u) for u in pair]
            if pair[0] == N - LEAD:
                for u in range(STEP):
                    soften(N - STEP + u)
                pack_last()
            for u, o in zip(pair, os):
                if u < owned:
                    keep(u, o)
                else:
                    keep_last(u, o)
            for u in pair:
                if u < owned:
                    send_part(u)
            if pair[0] == N - LEAD:
                spread(xst, 1)

    spread(x16, 0)
    pl.when(me < owned)(own)
    all_of(xst, x_recv.at[1])
    shares_last()
    all_of(x16, x_recv.at[0])
    merge_last()

    def blocks(ref, count, sem):
        run = ref.at[pl.ds(0, count)]
        pltpu.make_async_copy(run, run, sem).wait()

    @pl.when(me < owned)
    def _():
        blocks(o_ref, n - 1, b_send)
        blocks(o_ref, owned - 1, b_recv)
        blocks(msg, owned - 1, p_send)

    @pl.when(me >= owned)
    def _():
        blocks(o_ref, owned, b_recv)
        blocks(msg, owned, p_send)

    all_of(x16, x_send.at[0])
    all_of(xst, x_send.at[1])


def solution(mesh):
    n = mesh.shape["sp"]

    def step(q, k, v):
        N, tokens, heads, head = k.shape
        halves = heads // ROWS
        flat = (N, tokens * heads, head)
        bf16, f32 = jnp.bfloat16, jnp.float32
        dma = pltpu.SemaphoreType.DMA
        out = pl.pallas_call(
            functools.partial(kernel, n),
            out_shape=pltpu.VMEM((N, halves, ROWS, head), bf16),
            in_specs=[pl.BlockSpec(memory_space=pl.ANY)] * 3,
            out_specs=pl.BlockSpec(memory_space=pltpu.VMEM),
            scratch_shapes=[
                pltpu.VMEM((N, heads, head), bf16),
                pltpu.VMEM((KEYS, tokens * heads, head), bf16),
                pltpu.VMEM((SLOTS, tokens * heads, head), bf16),
                pltpu.VMEM((2 * STEP, heads, tokens * heads), f32),
                pltpu.VMEM((LEAD, heads, tokens * heads), bf16),
                pltpu.VMEM((N, ROWS, LANES), f32),
                pltpu.VMEM((N, halves + 1, ROWS, LANES), f32),
                pltpu.VMEM((n, halves + 1, ROWS, LANES), f32),
                pltpu.VMEM((n, LAST, halves, ROWS, head), bf16),
                pltpu.VMEM((n, ROWS, LANES), f32),
                pltpu.VMEM((n, LAST, halves, ROWS, LANES), f32),
                dma(()),
                dma((KEYS,)),
                dma((SLOTS,)),
                *[dma(())] * 4,
                dma((2,)),
                dma((2,)),
            ],
            compiler_params=pltpu.CompilerParams(collective_id=0, has_side_effects=True, vmem_limit_bytes=60 * 2**20),
        )(q, k.reshape(flat), v.reshape(flat))
        return out.reshape(q.shape)

    return jax.shard_map(
        step,
        mesh=mesh,
        in_specs=(P("dp", None, None), P("dp", "sp", None, None), P("dp", "sp", None, None)),
        out_specs=P("dp", None, None),
        check_vma=False,
    )
```
